32 devices in a mesh: zero: 8 (over z, x), model: 4 (over y, core).
Axes of the slice: x: 2, y: 2, z: 4, core: 2. Of those that a mesh axis runs over, the one named last changes fastest.
Arguments:
- w_query: bfloat16 [4096, 4096], P('zero', 'model'), may hold values from -0.125 to 0.125
- low_query: bfloat16 [4096, 16], P('zero'), may hold values from -0.09375 to 0.09375
- high_query: bfloat16 [16, 4096], P(None, 'model'), may hold values from -1.5 to 1.5
- w_key: bfloat16 [4096, 4096], P('zero', 'model'), may hold values from -0.125 to 0.125
- low_key: bfloat16 [4096, 16], P('zero'), may hold values from -0.09375 to 0.09375
- high_key: bfloat16 [16, 4096], P(None, 'model'), may hold values from -1.5 to 1.5
- w_value: bfloat16 [4096, 4096], P('zero', 'model'), may hold values from -0.125 to 0.125
- low_value: bfloat16 [4096, 16], P('zero'), may hold values from -0.09375 to 0.09375
- high_value: bfloat16 [16, 4096], P(None, 'model'), may hold values from -1.5 to 1.5
- norm_train: float32 [4096], P(('zero', 'model')), may hold values from 0.25 to 1.75
- norm_step: float32 [4096], P(('zero', 'model')), may hold values from -0.3 to 0.3
Outputs:
- serving_query: bfloat16 [4096, 4096], P(None, 'model')
- serving_key: bfloat16 [4096, 4096], P(None, 'model')
- serving_value: bfloat16 [4096, 4096], P(None, 'model')
- factor_query: float32 [4096], P('model')
- factor_key: float32 [4096], P('model')
- factor_value: float32 [4096], P('model')
- serve_norm: bfloat16 [4096], replicated
The draws below stay inside these ranges and needn't reach their ends.
All inputs are finite; a program needn't handle non-finite values. Where the reference program divides by a largest or mean magnitude, that divisor is 1e-20 or more.
Results may differ from the reference program's by a relative error of at most 0.001.
Values may be sent and summed in bfloat16 or wider, within the bound.
No kernel may reach another device: no remote copies, remote signals or barrier semaphores. Data moves between devices by JAX's collectives and lax.ppermute only.
A program may use at most 128 MiB of HBM per device.

```python
import jax
import jax.numpy as jnp

D_MODEL = 4096
Q_DIM = 4096
KV_DIM = 4096
RANK = 16


def spiked(array, stream_key, source, target, parts, factor):
    def block_of(axis_at):
        return (jnp.arange(array.shape[axis_at]) // (array.shape[axis_at] // parts)).reshape((-1,) + (1,) * (array.ndim - 1 - axis_at))

    first = jax.random.permutation(stream_key, parts)[block_of(target)]
    other_side = (block_of(target) + parts // 2) % parts
    return jnp.where((block_of(source) == first) | (block_of(source) == other_side), factor * array, array)


def block_levels(key, dims, cuts, least, largest):
    loudness = 1.0
    for axis_at, parts in cuts:
        heights = jax.random.uniform(jax.random.fold_in(jax.random.fold_in(key, 6), axis_at), (parts,), jnp.float32, least / len(cuts), largest / len(cuts))
        loudness = loudness * jnp.repeat(jnp.exp(heights), dims[axis_at] // parts).reshape((-1,) + (1,) * (len(dims) - 1 - axis_at))
    return loudness


def noise(own_key, extent, width, bound, cuts=(), kind=jnp.bfloat16):
    array = width * jax.random.normal(own_key, extent, jnp.float32)
    if cuts:
        array = array * block_levels(own_key, extent, cuts, -0.22, 0.18)
    return jnp.clip(array, -bound, bound).astype(kind)


def bell_draw_with(rng, extent, scale, reach, pieces, heavy, held_as=jnp.bfloat16):
    drawn = scale * jax.random.normal(rng, extent, jnp.float32)
    if pieces:
        drawn = drawn * block_levels(rng, extent, pieces, -0.22, 0.18)
    return jnp.clip(spiked(drawn, jax.random.fold_in(rng, 3), *heavy), -reach, reach).astype(held_as)


def setup_inputs(seed: int = 0) -> dict:
    key_list = jax.random.split(jax.random.key(seed), 12)
    return {
        "w_query": bell_draw_with(key_list[0], (D_MODEL, Q_DIM), D_MODEL ** -0.5, 0.125, ((0, 8), (1, 4)), (0, 1, 8, 2.0)),
        "low_query": noise(key_list[1], (D_MODEL, RANK), D_MODEL ** -0.5, 0.09375, ((0, 8),)),
        "high_query": noise(key_list[2], (RANK, Q_DIM), RANK ** -0.5, 1.5, ((1, 4),)),
        "w_key": bell_draw_with(key_list[3], (D_MODEL, KV_DIM), D_MODEL ** -0.5, 0.125, ((0, 8), (1, 4)), (0, 1, 8, 2.0)),
        "low_key": noise(key_list[4], (D_MODEL, RANK), D_MODEL ** -0.5, 0.09375, ((0, 8),)),
        "high_key": noise(key_list[5], (RANK, KV_DIM), RANK ** -0.5, 1.5, ((1, 4),)),
        "w_value": bell_draw_with(key_list[6], (D_MODEL, KV_DIM), D_MODEL ** -0.5, 0.125, ((0, 8), (1, 4)), (0, 1, 8, 2.0)),
        "low_value": noise(key_list[7], (D_MODEL, RANK), D_MODEL ** -0.5, 0.09375, ((0, 8),)),
        "high_value": noise(key_list[8], (RANK, KV_DIM), RANK ** -0.5, 1.5, ((1, 4),)),
        "norm_train": jnp.clip(1.0 + 0.15 * jax.random.normal(key_list[9], (D_MODEL,), jnp.float32), 0.25, 1.75),
        "norm_step": jnp.clip(jax.random.uniform(key_list[10], (D_MODEL,), jnp.float32, -0.3, 0.3) * block_levels(key_list[10], (D_MODEL,), ((0, 32),), -0.4, 0.0), -0.3, 0.3),
    }


mix_rate = 0.5


def reference(w_query, low_query, high_query, w_key, low_key, high_key, w_value, low_value, high_value, norm_train, norm_step):
    whole_query = w_query.astype(jnp.float32) + mix_rate * jnp.dot(low_query, high_query, preferred_element_type=jnp.float32)
    whole_key = w_key.astype(jnp.float32) + mix_rate * jnp.dot(low_key, high_key, preferred_element_type=jnp.float32)
    whole_value = w_value.astype(jnp.float32) + mix_rate * jnp.dot(low_value, high_value, preferred_element_type=jnp.float32)
    factor_query = jnp.sum(jnp.abs(whole_query), axis=0) / D_MODEL
    serving_query = (whole_query / factor_query).astype(jnp.bfloat16)
    factor_key = jnp.sum(jnp.abs(whole_key), axis=0) / D_MODEL
    serving_key = (whole_key / factor_key).astype(jnp.bfloat16)
    factor_value = jnp.sum(jnp.abs(whole_value), axis=0) / D_MODEL
    serving_value = (whole_value / factor_value).astype(jnp.bfloat16)
    serve_norm = (norm_train + norm_step).astype(jnp.bfloat16)
    return serving_query, serving_key, serving_value, factor_query, factor_key, factor_value, serve_norm
```

```python
import jax
import jax.numpy as jnp
from jax import lax
from jax.experimental import pallas as pl
from jax.experimental.pallas import tpu as pltpu
from jax.sharding import PartitionSpec as P

MIX_RATE = 0.5


def finish_kernel(members, rank, which, first_col, aliased):
    def kernel(*refs):
        refs = list(refs)
        starts = refs.pop(0)
        tops = [refs.pop(0) for _ in range(members)]
        bottoms = [refs.pop(0) for _ in range(members)]
        lows = [refs.pop(0) for _ in range(members)]
        high = refs.pop(0)
        if aliased:
            refs.pop(0)
        out, factor, held, whole, in_sems, out_sems = refs
        rows, cols = held.shape[1:]
        half = rows // 2
        step = min(128, rows)
        loads = []
        for s in range(members):
            pair = (
                pltpu.make_async_copy(tops[s], held.at[s, pl.ds(0, half)], in_sems.at[s, 0]),
                pltpu.make_async_copy(bottoms[s], held.at[s, pl.ds(half, half)], in_sems.at[s, 1]),
            )
            for copy in pair:
                copy.start()
            loads.append(pair)
        high_part = high[...]
        total = jnp.zeros((8, cols), jnp.float32)
        for s in range(members):
            for copy in loads[s]:
                copy.wait()
            for r in range(0, rows, step):
                low_part = lows[s][which * rank : (which + 1) * rank, r : r + step]
                product = lax.dot_general(
                    low_part,
                    high_part,
                    (((0,), (0,)), ((), ())),
                    preferred_element_type=jnp.float32,
                )
                value = held[s, r : r + step, :].astype(jnp.float32) + MIX_RATE * product
                whole[s, r : r + step, :] = value
                total = total + jnp.sum(jnp.abs(value).reshape(step // 8, 8, cols), axis=0)
        mean = jnp.sum(total, axis=0, keepdims=True) / (members * rows)
        factor[...] = mean
        scale = 1.0 / mean
        stores = []
        for s in range(members):
            for r in range(0, rows, step):
                held[s, r : r + step, :] = (whole[s, r : r + step, :] * scale).astype(jnp.bfloat16)
            copy = pltpu.make_async_copy(
                held.at[s],
                out.at[pl.ds(pl.multiple_of(starts[s], rows), rows), pl.ds(first_col, cols)],
                out_sems.at[s],
            )
            copy.start()
            stores.append(copy)
        for copy in stores:
            copy.wait()

    return kernel


def finish(starts, tops, bottoms, lows, high, which, rank, first_col, width, into=None):
    members = len(tops)
    half, cols = tops[0].shape
    rows = 2 * half
    hbm = pl.BlockSpec(memory_space=pl.ANY)
    vmem = pl.BlockSpec(memory_space=pltpu.VMEM)
    operands = [starts, *tops, *bottoms, *lows, high]
    specs = [pl.BlockSpec(memory_space=pltpu.SMEM)] + [hbm] * (2 * members) + [vmem] * (members + 1)
    aliases = {}
    if into is not None:
        aliases = {len(operands): 0}
        operands.append(into)
        specs.append(hbm)
    return pl.pallas_call(
        finish_kernel(members, rank, which, first_col, into is not None),
        out_shape=(
            jax.ShapeDtypeStruct((members * rows, width), jnp.bfloat16),
            jax.ShapeDtypeStruct((1, cols), jnp.float32),
        ),
        in_specs=specs,
        out_specs=(hbm, vmem),
        scratch_shapes=[
            pltpu.VMEM((members, rows, cols), jnp.bfloat16),
            pltpu.VMEM((members, rows, cols), jnp.float32),
            pltpu.SemaphoreType.DMA((members, 2)),
            pltpu.SemaphoreType.DMA((members,)),
        ],
        input_output_aliases=aliases,
        name=f"finish_{which}_{first_col}",
    )(*operands)


def after(value, *earlier):
    return lax.optimization_barrier((value, *earlier))[0]


def solution(mesh):
    members = mesh.shape["zero"]
    models = mesh.shape["model"]
    ring = list(range(0, members, 2)) + list(range(members - 1, 0, -2))
    place_of = [ring.index(m) for m in range(members)]

    def shift(s):
        return [(ring[p], ring[(p + s) % members]) for p in range(members)]

    onward, back = shift(1), shift(members - 1)

    def per_device(
        w_query, low_query, high_query, w_key, low_key, high_key,
        w_value, low_value, high_value, norm_train, norm_step,
    ):
        rows, width = w_query.shape
        half = rows // 2
        rank = low_query.shape[1]
        cut = width // 2
        place = jnp.asarray(place_of, jnp.int32)[lax.axis_index("zero")]
        origin = jnp.asarray(ring, jnp.int32)[(place - jnp.arange(members)) % members]
        starts = origin * rows

        chains = {
            "q": w_query,
            "k": w_key,
            "a": w_value[:, :cut],
            "b": w_value[:, cut:],
        }
        tops = {c: [w[:half]] for c, w in chains.items()}
        bottoms = {c: [w[half:]] for c, w in chains.items()}

        turns = []
        for pair in ("qk", "ab"):
            for _ in range(members - 1):
                turns += list(pair)
        done = []
        lows = None
        ready = {}

        def collected(c):
            return tops[c], [bottoms[c][0]] + bottoms[c][:0:-1]

        def gather_small():
            norm = (norm_train + norm_step).astype(jnp.bfloat16).reshape(1, -1)
            mine = lax.axis_index("model")
            near = [norm]
            for m in range(1, models):
                near.append(lax.ppermute(norm, "model", [(j, (j + m) % models) for j in range(models)]))
            near = jnp.concatenate(near, axis=0)
            near = near[(mine - jnp.arange(models)) % models].reshape(1, -1)
            small = jnp.concatenate([low_query.T, low_key.T, low_value.T, near], axis=0)
            return small, [small] + [lax.ppermute(small, "zero", shift(s)) for s in range(1, members)]

        def finished(c):
            t, b = collected(c)
            if c == "q":
                return finish(starts, t, b, lows, high_query, 0, rank, 0, width)
            if c == "k":
                return finish(starts, t, b, lows, high_key, 1, rank, 0, width)
            if c == "a":
                return finish(starts, t, b, lows, high_value[:, :cut], 2, rank, 0, width)
            return finish(starts, t, b, lows, high_value[:, cut:], 2, rank, cut, width, into=ready["a"][0])

        small, lows = gather_small()
        for t, c in enumerate(turns):
            up, down = tops[c][-1], bottoms[c][-1]
            if len(tops[c]) == 1 and t >= 3:
                up, down = after((up, down), *done[t - 3])
            if c == "a" and len(tops[c]) == 2:
                up, down = after((up, down), ready["q"][1])
            if c == "a" and len(tops[c]) == 4:
                up, down = after((up, down), ready["k"][1])
            moved = lax.ppermute(up, "zero", onward), lax.ppermute(down, "zero", back)
            tops[c].append(moved[0])
            bottoms[c].append(moved[1])
            done.append(moved)
            if len(tops[c]) == members and c != "b":
                ready[c] = finished(c)
        ready["b"] = finished("b")

        norms = jnp.stack([x[-1] for x in lows], axis=0)
        serve_norm = norms[(place - jnp.asarray(place_of, jnp.int32)) % members].reshape(-1)
        return (
            ready["q"][0],
            ready["k"][0],
            ready["b"][0],
            ready["q"][1].reshape(-1),
            ready["k"][1].reshape(-1),
            jnp.concatenate([ready["a"][1], ready["b"][1]], axis=1).reshape(-1),
            serve_norm,
        )

    return jax.shard_map(
        per_device,
        mesh=mesh,
        in_specs=(
            P("zero", "model"), P("zero", None), P(None, "model"),
            P("zero", "model"), P("zero", None), P(None, "model"),
            P("zero", "model"), P("zero", None), P(None, "model"),
            P(("zero", "model")), P(("zero", "model")),
        ),
        out_specs=(
            P(None, "model"), P(None, "model"), P(None, "model"),
            P("model"), P("model"), P("model"), P(),
        ),
        check_vma=False,
    )
```

```python
import jax
import jax.numpy as jnp
from jax import lax
from jax.experimental import pallas as pl
from jax.experimental.pallas import tpu as pltpu
from jax.sharding import PartitionSpec as P


MIX_RATE = 0.5


HBM = pl.BlockSpec(memory_space=pl.ANY)
VMEM = pl.BlockSpec(memory_space=pltpu.VMEM)
SMEM = pl.BlockSpec(memory_space=pltpu.SMEM)


def merged_rows(held, extra, high, shape, s, h, r, step, column):
    _, rank = shape
    low_part = extra[s, h, :rank, column + r : column + r + step]
    product = lax.dot_general(
        low_part, high, (((0,), (0,)), ((), ())), preferred_element_type=jnp.float32
    )
    return held[s, h, r : r + step, :].astype(jnp.float32) + MIX_RATE * product


def finish(pieces, high, column, members, extra=None, partial=None, fresh=None, origin=None, norm=0):
    count = len(pieces)
    cols = pieces[0][0].shape[1]
    rank = high.shape[0]
    carried = extra is None
    half = pieces[0][0].shape[0] - (rank if carried else 0)
    step = min(128, half)
    full = origin is not None
    fresh = list(range(count)) if fresh is None else fresh

    operands = [p for pair in pieces for p in pair] + [high]
    specs = [HBM] * (2 * count) + [VMEM]
    for value, spec in ((extra, VMEM), (partial, VMEM), (origin, SMEM)):
        if value is not None:
            operands.append(value)
            specs.append(spec)
    if full:
        shapes = [
            jax.ShapeDtypeStruct((members * 2 * half, cols), jnp.bfloat16),
            jax.ShapeDtypeStruct((1, cols), jnp.float32),
        ]
        outs = [HBM, VMEM]
    else:
        shapes, outs = [jax.ShapeDtypeStruct((8, cols), jnp.float32)], [VMEM]
    if carried:
        shapes += [
            jax.ShapeDtypeStruct((members, 2, rank, cols), jnp.bfloat16),
            jax.ShapeDtypeStruct((members, norm), jnp.float32),
        ]
        outs += [VMEM, VMEM]
    scratch = [pltpu.VMEM((count, 2, half, cols), jnp.bfloat16), pltpu.SemaphoreType.DMA((count, 2))]
    if full:
        scratch += [
            pltpu.VMEM((len(fresh), 2, half, cols), jnp.float32),
            pltpu.SemaphoreType.DMA((count, 2)),
        ]
    if carried:
        scratch += [pltpu.SemaphoreType.DMA((count, 2))]

    def kernel(*refs):
        refs = list(refs)
        sources = [[refs.pop(0), refs.pop(0)] for _ in range(count)]
        high_ref = refs.pop(0)
        extra_ref = None if carried else refs.pop(0)
        partial_ref = refs.pop(0) if partial is not None else None
        origin_ref = refs.pop(0) if full else None
        if full:
            out, factor = refs.pop(0), refs.pop(0)
        else:
            total_ref = refs.pop(0)
        if carried:
            extra_ref, norm_ref = refs.pop(0), refs.pop(0)
        held, in_sems = refs.pop(0), refs.pop(0)
        if full:
            whole, out_sems = refs.pop(0), refs.pop(0)
        if carried:
            extra_sems = refs.pop(0)

        loads = {}
        for s in fresh + [s for s in range(count) if s not in fresh]:
            loads[s] = []
            for h in range(2):
                if carried:
                    loads[s].append(
                        pltpu.make_async_copy(
                            sources[s][h].at[pl.ds(half, rank)], extra_ref.at[s, h], extra_sems.at[s, h]
                        )
                    )
                loads[s].append(
                    pltpu.make_async_copy(
                        sources[s][h].at[pl.ds(0, half)], held.at[s, h], in_sems.at[s, h]
                    )
                )
            for copy in loads[s]:
                copy.start()
        high_part = high_ref[...]
        shape = (half, rank)
        total = jnp.zeros((8, cols), jnp.float32) if partial is None else partial_ref[...]
        for slot, s in enumerate(fresh):
            for copy in loads[s]:
                copy.wait()
            for h in range(2):
                for r in range(0, half, step):
                    value = merged_rows(held, extra_ref, high_part, shape, s, h, r, step, column)
                    if full:
                        whole[slot, h, r : r + step, :] = value
                    total = total + jnp.sum(jnp.abs(value).reshape(step // 8, 8, cols), axis=0)
        if not full:
            total_ref[...] = total
            return
        mean = jnp.sum(total, axis=0, keepdims=True) / (members * 2 * half)
        factor[...] = mean
        scale = 1.0 / mean
        stores = []
        for s in range(count):
            if s not in fresh:
                for copy in loads[s]:
                    copy.wait()
            for h in range(2):
                for r in range(0, half, step):
                    if s in fresh:
                        value = whole[fresh.index(s), h, r : r + step, :]
                    else:
                        value = merged_rows(held, extra_ref, high_part, shape, s, h, r, step, column)
                    held[s, h, r : r + step, :] = (value * scale).astype(jnp.bfloat16)
            first = pl.multiple_of(origin_ref[s] * (2 * half), 2 * half)
            pair = [
                pltpu.make_async_copy(
                    held.at[s, h], out.at[pl.ds(pl.multiple_of(first + h * half, half), half)], out_sems.at[s, h]
                )
                for h in range(2)
            ]
            stores.append(pair)
            for copy in pair:
                copy.start()
        if carried:
            spot = 3 * max(half, 128)
            for s in range(count):
                norm_ref[pl.ds(origin_ref[s], 1), :] = extra_ref[s, 0, 0:1, spot : spot + norm].astype(jnp.float32)
        for pair in stores:
            for copy in pair:
                copy.wait()

    return pl.pallas_call(
        kernel, out_shape=tuple(shapes), in_specs=specs, out_specs=tuple(outs), scratch_shapes=scratch
    )(*operands)


def after(value, *earlier):
    return lax.optimization_barrier((value, *earlier))[0]


def solution(mesh):
    members = mesh.shape["zero"]
    models = mesh.shape["model"]
    ring = list(range(0, members, 2)) + list(range(members - 1, 0, -2))
    place_of = [ring.index(m) for m in range(members)]
    onward = [(ring[p], ring[(p + 1) % members]) for p in range(members)]
    back = [(b, a) for a, b in onward]
    steps = members - 1
    lead = steps // 2
    turns = ["v", "q"] * lead + ["k", "q"] * (steps - lead) + ["v", "k"] * lead + ["v"]
    last = len(turns) - 1
    q_end = max(t for t, c in enumerate(turns) if c == "q")

    def per_device(
        w_query, low_query, high_query, w_key, low_key, high_key,
        w_value, low_value, high_value, norm_train, norm_step,
    ):
        rows, width = w_query.shape
        half = rows // 2
        rank = low_query.shape[1]
        stride = max(half, 128)
        norm_size = norm_train.shape[0]
        place = jnp.asarray(place_of, jnp.int32)[lax.axis_index("zero")]
        origin = jnp.asarray(ring, jnp.int32)[(place - jnp.arange(members)) % members]
        norm = (norm_train + norm_step).astype(jnp.bfloat16).reshape(1, -1)

        def below(h):
            parts = [low[h * half : (h + 1) * half].T for low in (low_query, low_key, low_value)]
            parts = [jnp.pad(p, ((0, 0), (0, stride - half))) for p in parts]
            parts.append(jnp.pad(norm, ((0, rank - 1), (0, width - 3 * stride - norm_size))))
            return jnp.concatenate(parts, axis=1)

        sent = {}
        sent["v"] = [[w_value[:half]], [w_value[half:]]]
        sent["q"] = [[jnp.concatenate([w_query[h * half : (h + 1) * half], below(h)], axis=0)] for h in range(2)]
        sent["k"] = [[w_key[:half]], [w_key[half:]]]

        def collected(c):
            top, bottom = sent[c]
            return [(top[s], bottom[(members - s) % members]) for s in range(members)]

        done = []
        result = {}
        last_at = {}
        for t, c in enumerate(turns):
            pair = (sent[c][0][-1], sent[c][1][-1])
            if t >= 2 and last_at.get(c) != t - 2:
                pair = after(pair, *done[t - 2])
            if t == q_end + 5:
                pair = after(pair, result["norm"])
            moved = lax.ppermute(pair[0], "zero", onward), lax.ppermute(pair[1], "zero", back)
            sent[c][0].append(moved[0])
            sent[c][1].append(moved[1])
            done.append(moved)
            last_at[c] = t
            if t == q_end:
                result["q"] = finish(collected("q"), high_query, 0, members, origin=origin, norm=norm_size)
                extra = result["q"][2]
                mine = lax.axis_index("model")
                near = result["q"][3].astype(jnp.bfloat16)
                gathered = [near] + [
                    lax.ppermute(near, "model", [(j, (j + m) % models) for j in range(models)])
                    for m in range(1, models)
                ]
                gathered = jnp.stack(gathered, axis=0)[(mine - jnp.arange(models)) % models]
                result["norm"] = jnp.swapaxes(gathered, 0, 1).reshape(-1)
            if t == last - 2:
                top, bottom = sent["v"]
                early = [s for s in range(members) if s not in (1, steps)]
                pieces = [(top[s], bottom[(members - s) % members]) for s in early]
                result["early"] = finish(
                    pieces, high_value, 2 * stride, members,
                    extra=jnp.concatenate([extra[0:1], extra[2:steps]], axis=0),
                )[0]
            if t == last - 1:
                result["k"] = finish(collected("k"), high_key, stride, members, extra=extra, origin=origin)
        result["v"] = finish(
            collected("v"), high_value, 2 * stride, members, extra=extra,
            partial=result["early"], fresh=[1, steps], origin=origin,
        )
        return (
            result["q"][0], result["k"][0], result["v"][0],
            result["q"][1].reshape(-1), result["k"][1].reshape(-1), result["v"][1].reshape(-1),
            result["norm"],
        )

    return jax.shard_map(
        per_device,
        mesh=mesh,
        in_specs=(
            P("zero", "model"), P("zero", None), P(None, "model"),
            P("zero", "model"), P("zero", None), P(None, "model"),
            P("zero", "model"), P("zero", None), P(None, "model"),
            P(("zero", "model")), P(("zero", "model")),
        ),
        out_specs=(
            P(None, "model"), P(None, "model"), P(None, "model"),
            P("model"), P("model"), P("model"), P(),
        ),
        check_vma=False,
    )
```
